32 devices in a mesh: row: 8 (over z, x), col: 4 (over y, core).
Axes of the slice: x: 2, y: 2, z: 4, core: 2. Of those that a mesh axis runs over, the one named last changes fastest.
Arguments:
- gradients: bfloat16 [8, 4, 4, 64, 1536], P('row', 'col'), may hold values from -96 to 96
- token_counts: int32 [8, 4], P('row', 'col'), may hold values from 16 to 256
- row_groups: int32 [2, 8, 4], replicated, may hold values from 0 to 3, each once within a row
- col_groups: int32 [1, 4, 8], replicated, may hold values from 0 to 7, each once within a row
Outputs:
- averaged: float32 [8, 4, 4, 64, 1536], P('row', 'col')
- totals: int32 [8, 4], P('row', 'col')
The draws below stay inside these ranges and needn't reach their ends.
Inputs may be any that keep to these rules, and one draw needn't show every extreme that they name: row_groups[r, i] lists the 4 grid columns in some order: in row round r, grid row i's member of group g sits in column row_groups[r, i, g]. col_groups[0, j] lists the 8 grid rows in some order: grid column j's member of group h sits in row col_groups[0, j, h].
All inputs are finite; a program needn't handle non-finite values.
Results may differ from the reference program's by a relative error of at most 0.0003.
Values may be sent and summed in bfloat16 or wider, within the bound.
A program may use at most 64 MiB of HBM per device.

```python
import jax
import jax.numpy as jnp

D = 1536
BLOCKS = 4
GR = 64
N_ROW = 8
N_COL = 4


def with_ends(drawn, rng, smallest, largest):
    spot = [jax.random.randint(jax.random.fold_in(rng, axis), (), 0, length) for axis, length in enumerate(drawn.shape)]
    widest = drawn.shape.index(max(drawn.shape))
    beside = spot[:widest] + [(spot[widest] + 1) % drawn.shape[widest]] + spot[widest + 1:]
    return drawn.at[tuple(spot)].set(smallest).at[tuple(beside)].set(largest)


def block_scale(rng, dims, split, smallest, high):
    def one(dim, blocks):
        steps = jax.random.uniform(jax.random.fold_in(jax.random.fold_in(rng, 6), dim), (blocks,), jnp.float32, smallest / len(split), high / len(split))
        return jnp.repeat(jnp.exp(steps), dims[dim] // blocks).reshape((-1,) + (1,) * (len(dims) - dim - 1))

    level = one(*split[0])
    for cut in split[1:]:
        level = level * one(*cut)
    return level


def centred(rng, extent, deviation, reach, pieces=(), dtype=jnp.bfloat16):
    array = deviation * jax.random.normal(rng, extent, jnp.float32)
    if pieces:
        array = array * block_scale(rng, extent, pieces, -0.22, 0.18)
    return jnp.clip(array, -reach, reach).astype(dtype)


def setup_inputs(seed: int = 0) -> dict:
    seeds = jax.random.split(jax.random.key(seed), 5)
    return {
        "gradients": centred(seeds[0], (N_ROW, N_COL, BLOCKS, GR, D), 16.0, 96.0, ((0, 8), (1, 4))),
        "token_counts": with_ends(jax.random.randint(seeds[1], (N_ROW, N_COL), 16, 257), jax.random.fold_in(seeds[1], 1), 16, 256).astype(jnp.int32),
        "row_groups": jax.vmap(lambda own: jax.random.permutation(own, N_COL))(jax.random.split(seeds[2], 2 * N_ROW)).reshape((2, N_ROW, N_COL)).astype(jnp.int32),
        "col_groups": jax.vmap(lambda own: jax.random.permutation(own, N_ROW))(jax.random.split(seeds[3], 1 * N_COL)).reshape((1, N_COL, N_ROW)).astype(jnp.int32),
    }


def groups_average(values, weights, group_order):
    picked = jnp.take_along_axis(values, group_order[:, :, None, None], axis=1)
    picked_w = jnp.take_along_axis(weights, group_order, axis=1)
    group_sums = jnp.sum(picked * picked_w[:, :, None, None], axis=0)
    group_totals = jnp.sum(picked_w, axis=0)
    averaged = group_sums / group_totals[:, None, None]
    inverse = jnp.argsort(group_order, axis=1).astype(jnp.int32)
    return averaged[inverse], group_totals[inverse]


def reference(gradients, token_counts, row_groups, col_groups):
    grad_state = gradients.reshape(N_ROW, N_COL, BLOCKS * GR, D).astype(jnp.float32)
    weight = token_counts.astype(jnp.float32)
    grad_state, weight = groups_average(grad_state, weight, row_groups[0])
    swapped, swapped_w = groups_average(jnp.swapaxes(grad_state, 0, 1), weight.T, col_groups[0])
    grad_state = jnp.swapaxes(swapped, 0, 1)
    weight = swapped_w.T
    grad_state, weight = groups_average(grad_state, weight, row_groups[1])
    return grad_state.reshape(gradients.shape), weight.astype(jnp.int32)
```

```python
import functools

import jax
import jax.numpy as jnp
from jax import lax
from jax.experimental import pallas as pl
from jax.experimental.pallas import tpu as pltpu
from jax.sharding import PartitionSpec as P

MESH = pl.DeviceIdType.MESH
F32 = jnp.float32
WIDE = 256
LEAD = 6.5
CROSS_LAG = 2.2
RETURN_LAG = 4.3
VMEM_GRANT = 48 * 1024 * 1024
LIMIT = 32766.0
FINE = 524200.0
SMALLEST = 1e-33


def add(one, two):
    return one + two


def path_counts(cols, table, between, second, third, paths):
    hops = between.shape[2]

    @pl.loop(0, hops)
    def _(h):
        for g in range(cols):
            for turn, into in ((0, second), (1, third)):
                into[h, g] = functools.reduce(add, [
                    (table[turn, g, between[0, j, h]] == j).astype(jnp.int32) for j in range(cols)])

    @pl.loop(0, cols)
    def _(k):
        for g in range(cols):
            paths[k, g] = functools.reduce(add, [third[h, k] * second[h, g] for h in range(hops)])


def group_of(table, turn, row, col, cols):
    found = jnp.int32(0)
    for g in range(cols):
        found = jnp.where(table[turn, g, row] == col, g, found)
    return found


def encode(sums, k, code_ref, step_ref):
    groups = len(sums)
    for low in range(0, groups, 4):
        packed = None
        for g in range(low, min(low + 4, groups)):
            part = sums[g]
            step = jnp.maximum(jnp.max(jnp.abs(part), axis=0, keepdims=True), SMALLEST) * (1.0 / FINE)
            step_ref[k, g] = step
            code = jnp.round(part * (1.0 / step)).astype(jnp.int32)
            code_ref[k, g] = (code >> 4).astype(jnp.int16)
            bits = (code & 15) << (4 * (g - low))
            packed = bits if packed is None else packed + bits
        code_ref[k, groups + low // 4] = (packed - 32768).astype(jnp.int16)


def decode(groups, code_ref, step_ref):
    values = []
    for low in range(0, groups, 4):
        packed = code_ref[groups + low // 4].astype(jnp.int32) + 32768
        for g in range(low, min(low + 4, groups)):
            code = code_ref[g].astype(jnp.int32) * 16 + ((packed >> (4 * (g - low))) & 15)
            values.append(code.astype(F32) * step_ref[g])
    return values


def kernel(
    geometry,
    table_hbm, between_hbm, count_ref, x_hbm,
    out_ref, scale_ref, total_ref,
    table, between, x_ref,
    recv, own, cross_out, cross_out_step, cross_in, cross_in_step,
    codes, steps, twin_in, twin_in_step, pick, pick_step, ret, ret_scale,
    cnt_out, cnt_in, part_out, part_in, weights, inverse, factor,
    second, third, paths,
    load_sem, x_send_sem, x_recv_sem, n_send_sem, n_recv_sem, p_send_sem, p_recv_sem,
    c_send_sem, c_recv_sem, cs_recv_sem, t_send_sem, t_recv_sem, ts_recv_sem,
    cs_send_sem, ts_send_sem, r_send_sem, r_recv_sem, s_send_sem, s_recv_sem,
):
    across, cols, depth, levels, chunks, wide = geometry
    plane, teams, groups = across * cols, depth // levels, cols
    crew = plane * levels
    row, col = lax.axis_index("row"), lax.axis_index("col")
    z = row // across
    team, deck = z // levels, z % levels
    spot = (row % across) * cols + col
    me = spot * levels + deck

    def at(level, q):
        return (level * across + q // cols, q % cols)

    def member(p):
        return at(team * levels + p % levels, p // levels)

    def fellow(q):
        return at(z, q)

    def ally(d):
        return at((team + d) % teams * levels + deck, spot)

    def twin(d):
        return at(team * levels + (deck + d) % levels, spot)

    def lanes(k):
        return pl.ds(k * wide, wide)

    def remote(src, dst, send_sem, recv_sem, device):
        return pltpu.make_async_remote_copy(
            src_ref=src, dst_ref=dst, send_sem=send_sem, recv_sem=recv_sem, device_id=device, device_id_type=MESH)

    loads = [
        pltpu.make_async_copy(src, dst, load_sem.at[n])
        for n, (src, dst) in enumerate(
            [(x_hbm, x_ref), (table_hbm, table), (between_hbm, between)])]
    for load in loads:
        load.start()

    barrier = pltpu.get_barrier_semaphore()
    for d in range(1, crew):
        pl.semaphore_signal(barrier, inc=1, device_id=member((me + d) % crew), device_id_type=MESH)
    for d in range(1, teams):
        pl.semaphore_signal(barrier, inc=1, device_id=ally(d), device_id_type=MESH)
    count = count_ref[0, 0].astype(F32)
    cnt_out[...] = jnp.full(cnt_out.shape, count, F32)
    loads[0].wait()
    pl.semaphore_wait(barrier, crew + teams - 2)

    def count_copy(d):
        return remote(cnt_out, cnt_in.at[d - 1], n_send_sem, n_recv_sem, member((me + d) % crew))

    def piece_copy(k, d):
        to = (me + d) % crew
        return remote(x_ref.at[to, :, lanes(k)], recv.at[k, d - 1], x_send_sem, x_recv_sem.at[k], member(to))

    def part_copy(d):
        return remote(part_out, part_in.at[d - 1], p_send_sem, p_recv_sem, ally(d))

    def cross_copies(k, d):
        return (
            remote(cross_out_step.at[k], cross_in_step.at[k, d - 1], cs_send_sem, cs_recv_sem.at[k], ally(d)),
            remote(cross_out.at[k], cross_in.at[k, d - 1], c_send_sem, c_recv_sem.at[k], ally(d)))

    def twin_copies(k, d):
        return (
            remote(steps.at[k], twin_in_step.at[k, d - 1], ts_send_sem, ts_recv_sem.at[k], twin(d)),
            remote(codes.at[k], twin_in.at[k, d - 1], t_send_sem, t_recv_sem.at[k], twin(d)))

    def return_copies(k, d):
        to = (spot + d) % plane
        return (
            remote(ret_scale.at[k, d - 1], scale_ref.at[spot, :, :, lanes(k)], s_send_sem, s_recv_sem, fellow(to)),
            remote(ret.at[k, d - 1], out_ref.at[spot, :, :, lanes(k)], r_send_sem, r_recv_sem, fellow(to)))

    def begin(k):
        for d in range(1, crew):
            piece_copy(k, d).start()

    def gather(k):
        remote(recv.at[k], recv.at[k], x_send_sem, x_recv_sem.at[k], member((me + 1) % crew)).wait_recv()
        sums = [None] * groups
        for d in range(crew):
            piece = (x_ref[me, :, lanes(k)] if d == 0 else recv[k, d - 1]).astype(F32)
            for g in range(groups):
                term = piece * factor[d, g]
                sums[g] = term if d == 0 else sums[g] + term
        for g in range(groups):
            own[k, g] = sums[g]
        if teams > 1:
            encode(sums, k, cross_out, cross_out_step)
            for d in range(1, teams):
                for copy in cross_copies(k, d):
                    copy.start()

    def settle():
        if teams > 1:
            remote(part_in, part_in, p_send_sem, p_recv_sem, ally(1)).wait_recv()
        for g in range(groups):
            weight = part_out[g]
            for d in range(1, teams):
                weight = weight + part_in[d - 1, g]
            weights[g] = weight
            inverse[g] = 1.0 / weight
        mine = group_of(table, 1, row, col, cols)
        total_ref[...] = weights[mine, :, :1].astype(jnp.int32)

    def cross(k):
        sums = [own[k, g] for g in range(groups)]
        if teams > 1:
            remote(cross_in_step.at[k], cross_in_step.at[k], cs_send_sem, cs_recv_sem.at[k], ally(1)).wait_recv()
            remote(cross_in.at[k], cross_in.at[k], c_send_sem, c_recv_sem.at[k], ally(1)).wait_recv()
        for d in range(1, teams):
            sums = [a + b for a, b in zip(sums, decode(groups, cross_in.at[k, d - 1], cross_in_step.at[k, d - 1]))]
        for g in range(groups):
            mean = sums[g] * inverse[g]
            step = jnp.maximum(jnp.max(jnp.abs(mean), axis=0, keepdims=True), SMALLEST) * (1.0 / LIMIT)
            steps[k, g] = step
            codes[k, g] = jnp.round(mean * (1.0 / step)).astype(jnp.int32).astype(jnp.int16)
        for d in range(1, levels):
            for copy in twin_copies(k, d):
                copy.start()

    def give(k):
        if levels > 1:
            remote(twin_in_step.at[k], twin_in_step.at[k], ts_send_sem, ts_recv_sem.at[k], twin(1)).wait_recv()
            remote(twin_in.at[k], twin_in.at[k], t_send_sem, t_recv_sem.at[k], twin(1)).wait_recv()
            for d in range(1, levels):
                for g in range(groups):
                    pick[d - 1, g] = twin_in[k, d - 1, g]
                    pick_step[d - 1, g] = twin_in_step[k, d - 1, g]
        for d in range(plane):
            g = group_of(table, 1, *fellow((spot + d) % plane), cols)
            for l in range(levels):
                code = codes[k, g] if l == 0 else pick[l - 1, g]
                step = steps[k, g] if l == 0 else pick_step[l - 1, g]
                home = (deck + levels - l) % levels
                if d == 0:
                    out_ref[spot, home, :, lanes(k)] = code
                    scale_ref[spot, home, :, lanes(k)] = step
                else:
                    ret[k, d - 1, home] = code
                    ret_scale[k, d - 1, home] = step
            if d > 0:
                for copy in return_copies(k, d):
                    copy.start()

    for d in range(1, crew):
        count_copy(d).start()
    plan = []
    for k in range(chunks):
        plan.append((k - LEAD, 0, begin, k))
        plan.append((k, 3, gather, k))
        plan.append((k + CROSS_LAG, 2, cross, k))
        plan.append((k + RETURN_LAG, 1, give, k))
    plan.sort(key=lambda entry: (entry[0], entry[1]))
    early = [entry for entry in plan if entry[0] < 0]
    for _, _, action, k in early:
        action(k)

    loads[1].wait()
    loads[2].wait()
    path_counts(cols, table, between, second, third, paths)
    remote(cnt_in, cnt_in, n_send_sem, n_recv_sem, member((me + 1) % crew)).wait_recv()
    parts = [None] * groups
    for d in range(crew):
        i, j = member((me + crew - d) % crew)
        first = group_of(table, 0, i, j, cols)
        tally = cnt_out[...] if d == 0 else cnt_in[d - 1]
        for g in range(groups):
            term = paths[g, first].astype(F32) * tally
            factor[d, g] = term
            parts[g] = term if d == 0 else parts[g] + term
    for g in range(groups):
        part_out[g] = parts[g]
    for d in range(1, teams):
        part_copy(d).start()

    settled = False
    for _, _, action, k in plan[len(early):]:
        if action is cross and not settled:
            settle()
            settled = True
        action(k)

    member_any, team_any, twin_any, fellow_any = member((me + 1) % crew), ally(1), twin(1), fellow((spot + 1) % plane)
    remote(cnt_in, cnt_in, n_send_sem, n_recv_sem, member_any).wait_send()
    remote(recv, recv, x_send_sem, x_recv_sem.at[0], member_any).wait_send()
    if teams > 1:
        remote(part_in, part_in, p_send_sem, p_recv_sem, team_any).wait_send()
        remote(cross_in_step, cross_in_step, cs_send_sem, cs_recv_sem.at[0], team_any).wait_send()
        remote(cross_in, cross_in, c_send_sem, c_recv_sem.at[0], team_any).wait_send()
    if levels > 1:
        remote(twin_in_step, twin_in_step, ts_send_sem, ts_recv_sem.at[0], twin_any).wait_send()
        remote(twin_in, twin_in, t_send_sem, t_recv_sem.at[0], twin_any).wait_send()
    scales = remote(ret_scale, scale_ref.at[pl.ds(0, plane - 1)], s_send_sem, s_recv_sem, fellow_any)
    results = remote(ret, out_ref.at[pl.ds(0, plane - 1)], r_send_sem, r_recv_sem, fellow_any)
    for arrival in (scales, results):
        arrival.wait_send()
        arrival.wait_recv()


def local(gradients, token_counts, row_groups, col_groups):
    rows, cols = lax.axis_size("row"), lax.axis_size("col")
    across = 2 if rows % 2 == 0 else 1
    depth, plane = rows // across, across * cols
    width = gradients.shape[-1]
    lines = gradients.size // width
    levels = 2 if depth % 2 == 0 and lines % (2 * plane * 16) == 0 else 1
    teams, crew = depth // levels, levels * plane
    height = lines // crew
    wide = WIDE if width % WIDE == 0 else width
    chunks = width // wide
    groups = cols
    pieces = gradients.reshape(crew, height, width)
    hbm = pl.BlockSpec(memory_space=pltpu.HBM)
    smem = pl.BlockSpec(memory_space=pltpu.SMEM)
    stay = functools.partial(pltpu.with_memory_space_constraint, memory_space=pltpu.HBM)
    vmem = pl.BlockSpec(memory_space=pltpu.VMEM)
    others, mates = max(teams - 1, 1), max(levels - 1, 1)
    coded = groups + pl.cdiv(groups, 4)
    sem = pltpu.SemaphoreType.DMA
    codes, scales, total = pl.pallas_call(
        functools.partial(kernel, (across, cols, depth, levels, chunks, wide)),
        out_shape=(
            jax.ShapeDtypeStruct((plane, levels, height, width), jnp.int16),
            jax.ShapeDtypeStruct((plane, levels, 1, width), F32),
            jax.ShapeDtypeStruct((1, 1), jnp.int32),
        ),
        in_specs=[hbm, hbm, smem, hbm],
        out_specs=(vmem, vmem, vmem),
        scratch_shapes=[
            pltpu.SMEM((2, cols, rows), jnp.int32),
            pltpu.SMEM((1, cols, rows), jnp.int32),
            pltpu.VMEM((crew, height, width), gradients.dtype),
            pltpu.VMEM((chunks, crew - 1, height, wide), gradients.dtype),
            pltpu.VMEM((chunks, groups, height, wide), F32),
            pltpu.VMEM((chunks, coded, height, wide), jnp.int16),
            pltpu.VMEM((chunks, groups, 1, wide), F32),
            pltpu.VMEM((chunks, others, coded, height, wide), jnp.int16),
            pltpu.VMEM((chunks, others, groups, 1, wide), F32),
            pltpu.VMEM((chunks, groups, height, wide), jnp.int16),
            pltpu.VMEM((chunks, groups, 1, wide), F32),
            pltpu.VMEM((chunks, mates, groups, height, wide), jnp.int16),
            pltpu.VMEM((chunks, mates, groups, 1, wide), F32),
            pltpu.VMEM((mates, groups, height, wide), jnp.int16),
            pltpu.VMEM((mates, groups, 1, wide), F32),
            pltpu.VMEM((chunks, plane - 1, levels, height, wide), jnp.int16),
            pltpu.VMEM((chunks, plane - 1, levels, 1, wide), F32),
            pltpu.VMEM((1, wide), F32),
            pltpu.VMEM((crew - 1, 1, wide), F32),
            pltpu.VMEM((groups, 1, wide), F32),
            pltpu.VMEM((others, groups, 1, wide), F32),
            pltpu.VMEM((groups, 1, wide), F32),
            pltpu.VMEM((groups, 1, wide), F32),
            pltpu.VMEM((crew, groups, 1, wide), F32),
            pltpu.SMEM((rows, groups), jnp.int32),
            pltpu.SMEM((rows, groups), jnp.int32),
            pltpu.SMEM((groups, groups), jnp.int32),
            sem((3,)), sem, sem((chunks,)), sem, sem, sem, sem,
            sem, sem((chunks,)), sem((chunks,)), sem, sem((chunks,)), sem((chunks,)),
            sem, sem, sem, sem, sem, sem,
        ],
        compiler_params=pltpu.CompilerParams(
            collective_id=0, has_side_effects=True, vmem_limit_bytes=VMEM_GRANT
        ),
    )(stay(jnp.swapaxes(row_groups, 1, 2)), stay(col_groups), token_counts, stay(pieces))
    averaged = codes.astype(F32) * scales
    return averaged.reshape(gradients.shape), total


def solution(mesh):
    placed = (P("row", "col", None, None, None), P("row", "col"), P(), P())
    return jax.shard_map(
        local,
        mesh=mesh,
        in_specs=placed,
        out_specs=(P("row", "col", None, None, None), P("row", "col")),
        check_vma=False,
    )
```

```python
import functools

import jax
import jax.numpy as jnp
from jax import lax
from jax.experimental import pallas as pl
from jax.experimental.pallas import tpu as pltpu
from jax.sharding import PartitionSpec as P

MESH = pl.DeviceIdType.MESH
F32 = jnp.float32
WIDE = 256
JOINED = ()
TWINNED = (0, 1)
LEAD = 6.5
JOIN_LAG = 2.2
CROSS_LAG = 2.6
TWIN_LAG = 2.2
VMEM_GRANT = 48 * 1024 * 1024
LIMIT = 32766.0
SMALLEST = 1e-33
LANES = 128


def add(one, two):
    return one + two


def path_counts(cols, table, between, second, third, paths):
    hops = between.shape[2]

    @pl.loop(0, hops)
    def _(h):
        for g in range(cols):
            for turn, into in ((0, second), (1, third)):
                into[h, g] = functools.reduce(add, [
                    (table[turn, g, between[0, j, h]] == j).astype(jnp.int32) for j in range(cols)])

    @pl.loop(0, cols)
    def _(k):
        for g in range(cols):
            paths[k, g] = functools.reduce(add, [third[h, k] * second[h, g] for h in range(hops)])


def group_of(table, turn, row, col, cols):
    found = jnp.int32(0)
    for g in range(cols):
        found = jnp.where(table[turn, g, row] == col, g, found)
    return found


def spread(row, wide):
    return jnp.concatenate([row] * (wide // LANES), axis=1)


def quantize(part):
    wide = part.shape[1]
    top = jnp.max(jnp.abs(part), axis=0, keepdims=True)
    top = functools.reduce(jnp.maximum, [top[:, low:low + LANES] for low in range(0, wide, LANES)])
    step = jnp.maximum(top, SMALLEST) * (1.0 / LIMIT)
    return jnp.round(part * spread(1.0 / step, wide)).astype(jnp.int32).astype(jnp.int16), step


def encode(sums, code_ref, step_ref):
    for g, part in enumerate(sums):
        code_ref[g], step_ref[g] = quantize(part)


def decode(groups, code_ref, step_ref):
    wide = code_ref.shape[-1]
    return [code_ref[g].astype(F32) * spread(step_ref[g], wide) for g in range(groups)]


def kernel(
    geometry,
    table_hbm, between_hbm, count_ref, x_hbm,
    out_ref, scale_ref, total_ref,
    table, between, x_ref,
    recv, recv_raw, own, join_out, join_out_step, join_in, join_in_step, cross_out, cross_out_step, cross_in, cross_in_step,
    codes, steps, ret, ret_scale, twin_out, twin_out_step, twin_in, twin_in_step, pick, pick_step, pair, pair_scale,
    cnt_out, cnt_in, deal_out, deal_in, weights, inverse, factor,
    second, third, paths, chosen,
    load_sem, x_send_sem, x_recv_sem, n_send_sem, n_recv_sem, d_send_sem, d_recv_sem,
    j_send_sem, j_recv_sem, js_send_sem, js_recv_sem,
    c_send_sem, c_recv_sem, cs_send_sem, cs_recv_sem, t_send_sem, t_recv_sem, ts_send_sem, ts_recv_sem,
    r_send_sem, r_recv_sem, s_send_sem, s_recv_sem, b_send_sem, b_recv_sem, bs_send_sem, bs_recv_sem,
):
    across, cols, depth, levels, chunks, joined, twinned, wide = geometry
    crew = levels * across * cols
    slot = {k: (joined.index(k) if k in joined else k - sum(j < k for j in joined)) for k in range(chunks)}
    berth = {k: (twinned.index(k) if k in twinned else k - sum(j < k for j in twinned)) for k in range(chunks)}
    plane, teams, groups = across * cols, depth // levels, cols
    row, col = lax.axis_index("row"), lax.axis_index("col")
    z = row // across
    team, deck = z // levels, z % levels
    spot = (row % across) * cols + col

    def at(level, q):
        return (level * across + q // cols, q % cols)

    def fellow(q):
        return at(z, q)

    def mate(n):
        return at(team * levels + (deck + n // plane) % levels, (spot + n) % plane)

    def ally(d):
        return at((team + d) % teams * levels + deck, spot)

    def twin(d):
        return at(team * levels + (deck + d) % levels, spot)

    def lanes(k):
        return pl.ds(k * wide, wide)

    def remote(src, dst, send_sem, recv_sem, device):
        return pltpu.make_async_remote_copy(
            src_ref=src, dst_ref=dst, send_sem=send_sem, recv_sem=recv_sem, device_id=device, device_id_type=MESH)

    loads = [
        pltpu.make_async_copy(src, dst, load_sem.at[n])
        for n, (src, dst) in enumerate(
            [(x_hbm, x_ref), (table_hbm, table), (between_hbm, between)])]
    for load in loads:
        load.start()

    barrier = pltpu.get_barrier_semaphore()
    for n in range(1, crew):
        pl.semaphore_signal(barrier, inc=1, device_id=mate(n), device_id_type=MESH)
    for d in range(1, teams):
        pl.semaphore_signal(barrier, inc=1, device_id=ally(d), device_id_type=MESH)
    cnt_out[...] = count_ref[...]
    loads[0].wait()
    pl.semaphore_wait(barrier, crew + teams - 2)

    def strips(k):
        return pl.ds(k * LANES, LANES)

    def count_copy(n):
        return remote(cnt_out, cnt_in.at[n - 1], n_send_sem, n_recv_sem, mate(n))

    def piece_copy(k, d):
        to = (spot + d) % plane
        return remote(x_ref.at[to, :, :, lanes(k)], recv.at[slot[k], d - 1], x_send_sem, x_recv_sem.at[k], fellow(to))

    def raw_copy(k, n):
        source = x_ref.at[(spot + n) % plane, (deck + n // plane) % levels, :, lanes(k)]
        return remote(source, recv_raw.at[slot[k], n - 1], x_send_sem, x_recv_sem.at[k], mate(n))

    def deal_copy(d):
        return remote(deal_out, deal_in.at[d - 1], d_send_sem, d_recv_sem, ally(d))

    def join_copies(k, d):
        return (
            remote(join_out_step.at[slot[k], d - 1], join_in_step.at[slot[k], d - 1], js_send_sem, js_recv_sem.at[slot[k]], twin(d)),
            remote(join_out.at[slot[k], d - 1], join_in.at[slot[k], d - 1], j_send_sem, j_recv_sem.at[slot[k]], twin(d)))

    def cross_copies(k, d):
        return (
            remote(cross_out_step.at[k], cross_in_step.at[k, d - 1], cs_send_sem, cs_recv_sem.at[k], ally(d)),
            remote(cross_out.at[k], cross_in.at[k, d - 1], c_send_sem, c_recv_sem.at[k], ally(d)))

    def return_copies(k, n):
        i = berth[k]
        return (
            remote(ret_scale.at[i, n - 1], scale_ref.at[spot, deck, :, strips(k)], s_send_sem, s_recv_sem, mate(n)),
            remote(ret.at[i, n - 1], out_ref.at[spot, deck, :, lanes(k)], r_send_sem, r_recv_sem, mate(n)))

    def twin_copies(k, d):
        i = berth[k]
        return (
            remote(twin_out_step.at[i], twin_in_step.at[i, d - 1], ts_send_sem, ts_recv_sem.at[i], twin(d)),
            remote(twin_out.at[i], twin_in.at[i, d - 1], t_send_sem, t_recv_sem.at[i], twin(d)))

    def pair_copies(k, d):
        i, to = berth[k], fellow((spot + d) % plane)
        return (
            remote(pair_scale.at[i, d - 1], scale_ref.at[spot, :, :, strips(k)], bs_send_sem, bs_recv_sem, to),
            remote(pair.at[i, d - 1], out_ref.at[spot, :, :, lanes(k)], b_send_sem, b_recv_sem, to))

    def begin(k):
        if k not in joined:
            for n in range(1, crew):
                raw_copy(k, n).start()
        else:
            for d in range(1, plane):
                piece_copy(k, d).start()

    def gather_raw(k):
        remote(recv_raw.at[slot[k]], recv_raw.at[slot[k]], x_send_sem, x_recv_sem.at[k], fellow_any).wait_recv()
        sums = weigh([x_ref[spot, deck, :, lanes(k)] if n == 0 else recv_raw[slot[k], n - 1] for n in range(crew)])
        for g in range(groups):
            own[k, g] = sums[g]
        send_cross(k, sums)

    def weigh(pieces):
        sums = [None] * groups
        for n, piece in enumerate(pieces):
            piece = piece.astype(F32)
            for g in range(groups):
                term = piece * factor[n, g]
                sums[g] = term if n == 0 else sums[g] + term
        return sums

    def send_cross(k, sums):
        if teams > 1:
            encode(sums, cross_out.at[k], cross_out_step.at[k])
            for d in range(1, teams):
                for copy in cross_copies(k, d):
                    copy.start()

    def gather(k):
        remote(recv.at[slot[k]], recv.at[slot[k]], x_send_sem, x_recv_sem.at[k], fellow_any).wait_recv()
        for o in reversed(range(levels)):
            rows = (deck + o) % levels
            sums = weigh(
                [x_ref[spot, rows, :, lanes(k)] if d == 0 else recv[slot[k], d - 1, rows] for d in range(plane)])
            if o > 0:
                encode(sums, join_out.at[slot[k], o - 1], join_out_step.at[slot[k], o - 1])
                for copy in join_copies(k, o):
                    copy.start()
            else:
                for g in range(groups):
                    own[k, g] = sums[g]

    def join(k):
        sums = [own[k, g] for g in range(groups)]
        if levels > 1:
            remote(join_in_step.at[slot[k]], join_in_step.at[slot[k]], js_send_sem, js_recv_sem.at[slot[k]], twin(1)).wait_recv()
            remote(join_in.at[slot[k]], join_in.at[slot[k]], j_send_sem, j_recv_sem.at[slot[k]], twin(1)).wait_recv()
            for d in range(1, levels):
                sums = [a + b for a, b in zip(sums, decode(groups, join_in.at[slot[k], d - 1], join_in_step.at[slot[k], d - 1]))]
            for g in range(groups):
                own[k, g] = sums[g]
        send_cross(k, sums)

    def settle():
        if teams > 1:
            remote(deal_in, deal_in, d_send_sem, d_recv_sem, ally(1)).wait_recv()
        for g in range(groups):
            weight = deal_out[g]
            for d in range(1, teams):
                weight = weight + deal_in[d - 1, g]
            weights[g] = weight
            inverse[g] = 1.0 / weight
        total_ref[...] = weights[chosen[0]]

    def cross(k):
        sums = [own[k, g] for g in range(groups)]
        if teams > 1:
            remote(cross_in_step.at[k], cross_in_step.at[k], cs_send_sem, cs_recv_sem.at[k], ally(1)).wait_recv()
            remote(cross_in.at[k], cross_in.at[k], c_send_sem, c_recv_sem.at[k], ally(1)).wait_recv()
        for d in range(1, teams):
            sums = [a + b for a, b in zip(sums, decode(groups, cross_in.at[k, d - 1], cross_in_step.at[k, d - 1]))]
        i = berth[k]
        for g in range(groups):
            code, step = quantize(sums[g] * spread(inverse[g], wide))
            if k in twinned:
                twin_out[i, g], twin_out_step[i, g] = code, step
            else:
                codes[g], steps[g] = code, step
        if k in twinned:
            for d in range(1, levels):
                for copy in twin_copies(k, d):
                    copy.start()
            return
        for n in range(1, crew):
            ret[i, n - 1] = codes[chosen[n]]
            ret_scale[i, n - 1] = steps[chosen[n]]
            for copy in return_copies(k, n):
                copy.start()
        out_ref[spot, deck, :, lanes(k)] = codes[chosen[0]]
        scale_ref[spot, deck, :, strips(k)] = steps[chosen[0]]

    def give(k):
        i = berth[k]
        remote(twin_in_step.at[i], twin_in_step.at[i], ts_send_sem, ts_recv_sem.at[i], twin(1)).wait_recv()
        remote(twin_in.at[i], twin_in.at[i], t_send_sem, t_recv_sem.at[i], twin(1)).wait_recv()
        for g in range(groups):
            pick[0, g], pick_step[0, g] = twin_out[i, g], twin_out_step[i, g]
            for d in range(1, levels):
                pick[d, g], pick_step[d, g] = twin_in[i, d - 1, g], twin_in_step[i, d - 1, g]
        for d in range(plane):
            for l in range(levels):
                home = (deck + levels - l) % levels
                code, step = pick[l, chosen[d]], pick_step[l, chosen[d]]
                if d == 0:
                    out_ref[spot, home, :, lanes(k)] = code
                    scale_ref[spot, home, :, strips(k)] = step
                else:
                    pair[i, d - 1, home] = code
                    pair_scale[i, d - 1, home] = step
            if d > 0:
                for copy in pair_copies(k, d):
                    copy.start()

    fellow_any = fellow((spot + 1) % plane)
    for n in range(1, crew):
        count_copy(n).start()
    plan = []
    for k in range(chunks):
        plan.append((k - LEAD, 0, begin, k))
        lag = k
        if k in joined:
            plan.append((lag, 4, gather, k))
            lag += JOIN_LAG
            plan.append((lag, 3, join, k))
        else:
            plan.append((lag, 4, gather_raw, k))
        lag += CROSS_LAG
        plan.append((lag, 2, cross, k))
        if k in twinned:
            plan.append((lag + TWIN_LAG, 1, give, k))
    plan.sort(key=lambda entry: (entry[0], entry[1]))
    early = [entry for entry in plan if entry[0] < 0]
    for _, _, action, k in early:
        action(k)

    loads[1].wait()
    loads[2].wait()
    path_counts(cols, table, between, second, third, paths)
    remote(cnt_in, cnt_in, n_send_sem, n_recv_sem, fellow_any).wait_recv()
    for n in range(crew):
        chosen[n] = group_of(table, 1, *mate(n), cols)
    parts = [None] * groups
    for n in range(crew):
        i, j = at(team * levels + (deck + levels - n // plane) % levels, (spot + plane - n % plane) % plane)
        first = group_of(table, 0, i, j, cols)
        tally = cnt_out[...] if n == 0 else cnt_in[n - 1]
        for g in range(groups):
            term = paths[g, first].astype(F32) * tally
            factor[n, g] = spread(term, wide)
            parts[g] = term if n == 0 else parts[g] + term
    for g in range(groups):
        deal_out[g] = parts[g]
    for d in range(1, teams):
        deal_copy(d).start()

    seen = set()
    for _, _, action, k in plan[len(early):]:
        if action is cross and cross not in seen:
            settle()
        seen.add(action)
        action(k)

    remote(cnt_in, cnt_in, n_send_sem, n_recv_sem, fellow_any).wait_send()
    drains = []
    if len(joined) < chunks:
        drains.append((recv_raw, x_send_sem, x_recv_sem.at[0], fellow_any))
    if joined:
        drains += [
            (recv, x_send_sem, x_recv_sem.at[0], fellow_any), (join_in_step, js_send_sem, js_recv_sem.at[0], twin(1)),
            (join_in, j_send_sem, j_recv_sem.at[0], twin(1))]
    if teams > 1:
        drains += [
            (deal_in, d_send_sem, d_recv_sem, ally(1)), (cross_in_step, cs_send_sem, cs_recv_sem.at[0], ally(1)),
            (cross_in, c_send_sem, c_recv_sem.at[0], ally(1))]
    if twinned:
        drains += [
            (twin_in_step, ts_send_sem, ts_recv_sem.at[0], twin(1)), (twin_in, t_send_sem, t_recv_sem.at[0], twin(1))]
    for ref, send_sem, recv_sem, device in drains:
        remote(ref, ref, send_sem, recv_sem, device).wait_send()
    arrivals = []
    if len(twinned) < chunks:
        arrivals += [(ret_scale, s_send_sem, s_recv_sem), (ret, r_send_sem, r_recv_sem)]
    if twinned:
        arrivals += [(pair_scale, bs_send_sem, bs_recv_sem), (pair, b_send_sem, b_recv_sem)]
    for ref, send_sem, recv_sem in arrivals:
        remote(ref, ref, send_sem, recv_sem, fellow_any).wait_send()
        remote(ref, ref, send_sem, recv_sem, fellow_any).wait_recv()


def local(gradients, token_counts, row_groups, col_groups):
    rows, cols = lax.axis_size("row"), lax.axis_size("col")
    across = 2 if rows % 2 == 0 else 1
    depth, plane = rows // across, across * cols
    width = gradients.shape[-1]
    lines = gradients.size // width
    levels = 2 if depth % 2 == 0 and lines % (2 * plane * 16) == 0 else 1
    teams = depth // levels
    height = lines // (plane * levels)
    wide = WIDE if width % WIDE == 0 else LANES
    chunks = width // wide
    groups = cols
    counts = jnp.broadcast_to(token_counts.astype(F32), (1, LANES))
    pieces = gradients.reshape(plane, levels, height, width)
    hbm = pl.BlockSpec(memory_space=pltpu.HBM)
    stay = functools.partial(pltpu.with_memory_space_constraint, memory_space=pltpu.HBM)
    vmem = pl.BlockSpec(memory_space=pltpu.VMEM)
    others, mates = max(teams - 1, 1), max(levels - 1, 1)
    joined = tuple(k for k in JOINED if k < chunks and levels > 1)
    twinned = tuple(k for k in TWINNED if k < chunks and levels > 1)
    rest, raw = max(len(joined), 1), max(chunks - len(joined), 1)
    paired, single = max(len(twinned), 1), max(chunks - len(twinned), 1)
    crew = levels * plane
    sem = pltpu.SemaphoreType.DMA
    codes, scales, total = pl.pallas_call(
        functools.partial(kernel, (across, cols, depth, levels, chunks, joined, twinned, wide)),
        out_shape=(
            jax.ShapeDtypeStruct((plane, levels, height, width), jnp.int16),
            jax.ShapeDtypeStruct((plane, levels, 1, chunks * LANES), F32),
            jax.ShapeDtypeStruct((1, LANES), F32),
        ),
        in_specs=[hbm, hbm, vmem, hbm],
        out_specs=(vmem, vmem, vmem),
        scratch_shapes=[
            pltpu.SMEM((2, cols, rows), jnp.int32),
            pltpu.SMEM((1, cols, rows), jnp.int32),
            pltpu.VMEM((plane, levels, height, width), gradients.dtype),
            pltpu.VMEM((rest, plane - 1, levels, height, wide), gradients.dtype),
            pltpu.VMEM((raw, crew - 1, height, wide), gradients.dtype),
            pltpu.VMEM((chunks, groups, height, wide), F32),
            pltpu.VMEM((rest, mates, groups, height, wide), jnp.int16),
            pltpu.VMEM((rest, mates, groups, 1, LANES), F32),
            pltpu.VMEM((rest, mates, groups, height, wide), jnp.int16),
            pltpu.VMEM((rest, mates, groups, 1, LANES), F32),
            pltpu.VMEM((chunks, groups, height, wide), jnp.int16),
            pltpu.VMEM((chunks, groups, 1, LANES), F32),
            pltpu.VMEM((chunks, others, groups, height, wide), jnp.int16),
            pltpu.VMEM((chunks, others, groups, 1, LANES), F32),
            pltpu.VMEM((groups, height, wide), jnp.int16),
            pltpu.VMEM((groups, 1, LANES), F32),
            pltpu.VMEM((single, crew - 1, height, wide), jnp.int16),
            pltpu.VMEM((single, crew - 1, 1, LANES), F32),
            pltpu.VMEM((paired, groups, height, wide), jnp.int16),
            pltpu.VMEM((paired, groups, 1, LANES), F32),
            pltpu.VMEM((paired, mates, groups, height, wide), jnp.int16),
            pltpu.VMEM((paired, mates, groups, 1, LANES), F32),
            pltpu.VMEM((levels, groups, height, wide), jnp.int16),
            pltpu.VMEM((levels, groups, 1, LANES), F32),
            pltpu.VMEM((paired, plane - 1, levels, height, wide), jnp.int16),
            pltpu.VMEM((paired, plane - 1, levels, 1, LANES), F32),
            pltpu.VMEM((1, LANES), F32),
            pltpu.VMEM((crew - 1, 1, LANES), F32),
            pltpu.VMEM((groups, 1, LANES), F32),
            pltpu.VMEM((others, groups, 1, LANES), F32),
            pltpu.VMEM((groups, 1, LANES), F32),
            pltpu.VMEM((groups, 1, LANES), F32),
            pltpu.VMEM((crew, groups, 1, wide), F32),
            pltpu.SMEM((rows, groups), jnp.int32),
            pltpu.SMEM((rows, groups), jnp.int32),
            pltpu.SMEM((groups, groups), jnp.int32),
            pltpu.SMEM((crew,), jnp.int32),
            sem((3,)), sem, sem((chunks,)), sem, sem, sem, sem,
            sem, sem((rest,)), sem, sem((rest,)),
            sem, sem((chunks,)), sem, sem((chunks,)), sem, sem((paired,)), sem, sem((paired,)),
            sem, sem, sem, sem, sem, sem, sem, sem,
        ],
        compiler_params=pltpu.CompilerParams(
            collective_id=0, has_side_effects=True, vmem_limit_bytes=VMEM_GRANT
        ),
    )(stay(jnp.swapaxes(row_groups, 1, 2)), stay(col_groups), counts, stay(pieces))
    tiled = jnp.repeat(scales.reshape(plane, levels, 1, chunks, 1, LANES), wide // LANES, axis=4)
    averaged = codes.astype(F32) * tiled.reshape(plane, levels, 1, width)
    return averaged.reshape(gradients.shape), jnp.max(total.astype(jnp.int32), axis=1, keepdims=True)


def solution(mesh):
    placed = (P("row", "col", None, None, None), P("row", "col"), P(), P())
    return jax.shard_map(
        local,
        mesh=mesh,
        in_specs=placed,
        out_specs=(P("row", "col", None, None, None), P("row", "col")),
        check_vma=False,
    )
```

```python
import functools

import jax
import jax.numpy as jnp
from jax import lax
from jax.experimental import pallas as pl
from jax.experimental.pallas import tpu as pltpu
from jax.sharding import PartitionSpec as P

MESH = pl.DeviceIdType.MESH
F32 = jnp.float32
WIDE = 256
JOINED = ()
TWINNED = (0, 1)
LEAD = 6.5
FAR = 4.6
JOIN_LAG = 2.2
CROSS_LAG = 2.6
TWIN_LAG = 2.2
VMEM_GRANT = 48 * 1024 * 1024
LIMIT = 32766.0
SMALLEST = 1e-33
LANES = 128


def add(one, two):
    return one + two


def path_counts(cols, table, between, second, third, paths):
    hops = between.shape[2]

    @pl.loop(0, hops)
    def _(h):
        for g in range(cols):
            for turn, into in ((0, second), (1, third)):
                into[h, g] = functools.reduce(add, [
                    (table[turn, g, between[0, j, h]] == j).astype(jnp.int32) for j in range(cols)])

    @pl.loop(0, cols)
    def _(k):
        for g in range(cols):
            paths[k, g] = functools.reduce(add, [third[h, k] * second[h, g] for h in range(hops)])


def group_of(table, turn, row, col, cols):
    found = jnp.int32(0)
    for g in range(cols):
        found = jnp.where(table[turn, g, row] == col, g, found)
    return found


def spread(row, wide):
    return jnp.concatenate([row] * (wide // LANES), axis=1)


def quantize(part):
    wide = part.shape[1]
    top = jnp.max(jnp.abs(part), axis=0, keepdims=True)
    top = functools.reduce(jnp.maximum, [top[:, low:low + LANES] for low in range(0, wide, LANES)])
    step = jnp.maximum(top, SMALLEST) * (1.0 / LIMIT)
    return jnp.round(part * spread(1.0 / step, wide)).astype(jnp.int32).astype(jnp.int16), step


def encode(sums, code_ref, step_ref):
    for g, part in enumerate(sums):
        code_ref[g], step_ref[g] = quantize(part)


def decode(groups, code_ref, step_ref):
    wide = code_ref.shape[-1]
    return [code_ref[g].astype(F32) * spread(step_ref[g], wide) for g in range(groups)]


def kernel(
    geometry,
    table_hbm, between_hbm, count_ref, x_hbm,
    out_ref, spread_ref, total_ref,
    scale_ref, table, between, x_ref,
    recv, recv_raw, own, join_out, join_out_step, join_in, join_in_step, cross_out, cross_out_step, cross_in, cross_in_step,
    codes, steps, ret, ret_scale, twin_out, twin_out_step, twin_in, twin_in_step, pick, pick_step, pair, pair_scale,
    cnt_out, cnt_in, deal_out, deal_in, weights, inverse, factor,
    second, third, paths, chosen,
    load_sem, x_send_sem, x_recv_sem, n_send_sem, n_recv_sem, d_send_sem, d_recv_sem,
    j_send_sem, j_recv_sem, js_send_sem, js_recv_sem,
    c_send_sem, c_recv_sem, cs_send_sem, cs_recv_sem, t_send_sem, t_recv_sem, ts_send_sem, ts_recv_sem,
    r_send_sem, r_recv_sem, s_send_sem, s_recv_sem, b_send_sem, b_recv_sem, bs_send_sem, bs_recv_sem,
):
    across, cols, depth, levels, chunks, joined, twinned, wide = geometry
    crew = levels * across * cols
    slot = {k: (joined.index(k) if k in joined else k - sum(j < k for j in joined)) for k in range(chunks)}
    berth = {k: (twinned.index(k) if k in twinned else k - sum(j < k for j in twinned)) for k in range(chunks)}
    plane, teams, groups = across * cols, depth // levels, cols
    row, col = lax.axis_index("row"), lax.axis_index("col")
    z = row // across
    team, deck = z // levels, z % levels
    spot = (row % across) * cols + col

    def at(level, q):
        return (level * across + q // cols, q % cols)

    def fellow(q):
        return at(z, q)

    def mate(n):
        return at(team * levels + (deck + n // plane) % levels, (spot + n) % plane)

    def ally(d):
        return at((team + d) % teams * levels + deck, spot)

    def twin(d):
        return at(team * levels + (deck + d) % levels, spot)

    def lanes(k):
        return pl.ds(k * wide, wide)

    def remote(src, dst, send_sem, recv_sem, device):
        return pltpu.make_async_remote_copy(
            src_ref=src, dst_ref=dst, send_sem=send_sem, recv_sem=recv_sem, device_id=device, device_id_type=MESH)

    loads = [
        pltpu.make_async_copy(src, dst, load_sem.at[n])
        for n, (src, dst) in enumerate(
            [(x_hbm, x_ref), (table_hbm, table), (between_hbm, between)])]
    for load in loads:
        load.start()

    barrier = pltpu.get_barrier_semaphore()
    for n in range(1, crew):
        pl.semaphore_signal(barrier, inc=1, device_id=mate(n), device_id_type=MESH)
    for d in range(1, teams):
        pl.semaphore_signal(barrier, inc=1, device_id=ally(d), device_id_type=MESH)
    cnt_out[...] = count_ref[...]
    loads[0].wait()
    pl.semaphore_wait(barrier, crew + teams - 2)

    def strips(k):
        return pl.ds(k * LANES, LANES)

    def count_copy(n):
        return remote(cnt_out, cnt_in.at[n - 1], n_send_sem, n_recv_sem, mate(n))

    def piece_copy(k, d):
        to = (spot + d) % plane
        return remote(x_ref.at[to, :, :, lanes(k)], recv.at[slot[k], d - 1], x_send_sem, x_recv_sem.at[k], fellow(to))

    def raw_copy(k, n):
        source = x_ref.at[(spot + n) % plane, (deck + n // plane) % levels, :, lanes(k)]
        return remote(source, recv_raw.at[slot[k], n - 1], x_send_sem, x_recv_sem.at[k], mate(n))

    def deal_copy(d):
        return remote(deal_out, deal_in.at[d - 1], d_send_sem, d_recv_sem, ally(d))

    def join_copies(k, d):
        return (
            remote(join_out_step.at[slot[k], d - 1], join_in_step.at[slot[k], d - 1], js_send_sem, js_recv_sem.at[slot[k]], twin(d)),
            remote(join_out.at[slot[k], d - 1], join_in.at[slot[k], d - 1], j_send_sem, j_recv_sem.at[slot[k]], twin(d)))

    def cross_copies(k, d):
        return (
            remote(cross_out_step.at[k], cross_in_step.at[k, d - 1], cs_send_sem, cs_recv_sem.at[k], ally(d)),
            remote(cross_out.at[k], cross_in.at[k, d - 1], c_send_sem, c_recv_sem.at[k], ally(d)))

    def return_copies(k, n):
        i = berth[k]
        return (
            remote(ret_scale.at[i, n - 1], scale_ref.at[spot, deck, :, strips(k)], s_send_sem, s_recv_sem, mate(n)),
            remote(ret.at[i, n - 1], out_ref.at[spot, deck, :, lanes(k)], r_send_sem, r_recv_sem, mate(n)))

    def twin_copies(k, d):
        i = berth[k]
        return (
            remote(twin_out_step.at[i], twin_in_step.at[i, d - 1], ts_send_sem, ts_recv_sem.at[i], twin(d)),
            remote(twin_out.at[i], twin_in.at[i, d - 1], t_send_sem, t_recv_sem.at[i], twin(d)))

    def pair_copies(k, d):
        i, to = berth[k], fellow((spot + d) % plane)
        return (
            remote(pair_scale.at[i, d - 1], scale_ref.at[spot, :, :, strips(k)], bs_send_sem, bs_recv_sem, to),
            remote(pair.at[i, d - 1], out_ref.at[spot, :, :, lanes(k)], b_send_sem, b_recv_sem, to))

    def begin(k):
        if k not in joined:
            for n in range(1, plane):
                raw_copy(k, n).start()
        else:
            for d in range(1, plane):
                piece_copy(k, d).start()

    def begin_far(k):
        for n in range(plane, crew if k not in joined else 0):
            raw_copy(k, n).start()

    def gather_raw(k):
        remote(recv_raw.at[slot[k]], recv_raw.at[slot[k]], x_send_sem, x_recv_sem.at[k], fellow_any).wait_recv()
        sums = weigh([x_ref[spot, deck, :, lanes(k)] if n == 0 else recv_raw[slot[k], n - 1] for n in range(crew)])
        for g in range(groups):
            own[k, g] = sums[g]
        send_cross(k, sums)

    def weigh(pieces):
        sums = [None] * groups
        for n, piece in enumerate(pieces):
            piece = piece.astype(F32)
            for g in range(groups):
                term = piece * factor[n, g]
                sums[g] = term if n == 0 else sums[g] + term
        return sums

    def send_cross(k, sums):
        if teams > 1:
            encode(sums, cross_out.at[k], cross_out_step.at[k])
            for d in range(1, teams):
                for copy in cross_copies(k, d):
                    copy.start()

    def gather(k):
        remote(recv.at[slot[k]], recv.at[slot[k]], x_send_sem, x_recv_sem.at[k], fellow_any).wait_recv()
        for o in reversed(range(levels)):
            rows = (deck + o) % levels
            sums = weigh(
                [x_ref[spot, rows, :, lanes(k)] if d == 0 else recv[slot[k], d - 1, rows] for d in range(plane)])
            if o > 0:
                encode(sums, join_out.at[slot[k], o - 1], join_out_step.at[slot[k], o - 1])
                for copy in join_copies(k, o):
                    copy.start()
            else:
                for g in range(groups):
                    own[k, g] = sums[g]

    def join(k):
        sums = [own[k, g] for g in range(groups)]
        if levels > 1:
            remote(join_in_step.at[slot[k]], join_in_step.at[slot[k]], js_send_sem, js_recv_sem.at[slot[k]], twin(1)).wait_recv()
            remote(join_in.at[slot[k]], join_in.at[slot[k]], j_send_sem, j_recv_sem.at[slot[k]], twin(1)).wait_recv()
            for d in range(1, levels):
                sums = [a + b for a, b in zip(sums, decode(groups, join_in.at[slot[k], d - 1], join_in_step.at[slot[k], d - 1]))]
            for g in range(groups):
                own[k, g] = sums[g]
        send_cross(k, sums)

    def settle():
        if teams > 1:
            remote(deal_in, deal_in, d_send_sem, d_recv_sem, ally(1)).wait_recv()
        for g in range(groups):
            weight = deal_out[g]
            for d in range(1, teams):
                weight = weight + deal_in[d - 1, g]
            weights[g] = weight
            inverse[g] = 1.0 / weight
        total_ref[...] = weights[chosen[0]]

    def cross(k):
        sums = [own[k, g] for g in range(groups)]
        if teams > 1:
            remote(cross_in_step.at[k], cross_in_step.at[k], cs_send_sem, cs_recv_sem.at[k], ally(1)).wait_recv()
            remote(cross_in.at[k], cross_in.at[k], c_send_sem, c_recv_sem.at[k], ally(1)).wait_recv()
        for d in range(1, teams):
            sums = [a + b for a, b in zip(sums, decode(groups, cross_in.at[k, d - 1], cross_in_step.at[k, d - 1]))]
        i = berth[k]
        for g in range(groups):
            code, step = quantize(sums[g] * spread(inverse[g], wide))
            if k in twinned:
                twin_out[i, g], twin_out_step[i, g] = code, step
            else:
                codes[g], steps[g] = code, step
        if k in twinned:
            for d in range(1, levels):
                for copy in twin_copies(k, d):
                    copy.start()
            return
        for n in range(1, crew):
            ret[i, n - 1] = codes[chosen[n]]
            ret_scale[i, n - 1] = steps[chosen[n]]
            for copy in return_copies(k, n):
                copy.start()
        out_ref[spot, deck, :, lanes(k)] = codes[chosen[0]]
        scale_ref[spot, deck, :, strips(k)] = steps[chosen[0]]

    def give(k):
        i = berth[k]
        remote(twin_in_step.at[i], twin_in_step.at[i], ts_send_sem, ts_recv_sem.at[i], twin(1)).wait_recv()
        remote(twin_in.at[i], twin_in.at[i], t_send_sem, t_recv_sem.at[i], twin(1)).wait_recv()
        for g in range(groups):
            pick[0, g], pick_step[0, g] = twin_out[i, g], twin_out_step[i, g]
            for d in range(1, levels):
                pick[d, g], pick_step[d, g] = twin_in[i, d - 1, g], twin_in_step[i, d - 1, g]
        for d in range(plane):
            for l in range(levels):
                home = (deck + levels - l) % levels
                code, step = pick[l, chosen[d]], pick_step[l, chosen[d]]
                if d == 0:
                    out_ref[spot, home, :, lanes(k)] = code
                    scale_ref[spot, home, :, strips(k)] = step
                else:
                    pair[i, d - 1, home] = code
                    pair_scale[i, d - 1, home] = step
            if d > 0:
                for copy in pair_copies(k, d):
                    copy.start()

    fellow_any = fellow((spot + 1) % plane)
    for n in range(1, crew):
        count_copy(n).start()
    plan = []
    for k in range(chunks):
        plan.append((k - LEAD, 0, begin, k))
        plan.append((k - FAR, 0, begin_far, k))
        lag = k
        if k in joined:
            plan.append((lag, 4, gather, k))
            lag += JOIN_LAG
            plan.append((lag, 3, join, k))
        else:
            plan.append((lag, 4, gather_raw, k))
        lag += CROSS_LAG
        plan.append((lag, 2, cross, k))
        if k in twinned:
            plan.append((lag + TWIN_LAG, 1, give, k))
    plan.sort(key=lambda entry: (entry[0], entry[1]))
    early = [entry for entry in plan if entry[0] < 0]
    for _, _, action, k in early:
        action(k)

    loads[1].wait()
    loads[2].wait()
    path_counts(cols, table, between, second, third, paths)
    remote(cnt_in, cnt_in, n_send_sem, n_recv_sem, fellow_any).wait_recv()
    for n in range(crew):
        chosen[n] = group_of(table, 1, *mate(n), cols)
    parts = [None] * groups
    for n in range(crew):
        i, j = at(team * levels + (deck + levels - n // plane) % levels, (spot + plane - n % plane) % plane)
        first = group_of(table, 0, i, j, cols)
        tally = cnt_out[...] if n == 0 else cnt_in[n - 1]
        for g in range(groups):
            term = paths[g, first].astype(F32) * tally
            factor[n, g] = spread(term, wide)
            parts[g] = term if n == 0 else parts[g] + term
    for g in range(groups):
        deal_out[g] = parts[g]
    for d in range(1, teams):
        deal_copy(d).start()

    seen = set()
    for _, _, action, k in plan[len(early):]:
        if action is cross and cross not in seen:
            settle()
        seen.add(action)
        action(k)

    remote(cnt_in, cnt_in, n_send_sem, n_recv_sem, fellow_any).wait_send()
    drains = []
    if len(joined) < chunks:
        drains.append((recv_raw, x_send_sem, x_recv_sem.at[0], fellow_any))
    if joined:
        drains += [
            (recv, x_send_sem, x_recv_sem.at[0], fellow_any), (join_in_step, js_send_sem, js_recv_sem.at[0], twin(1)),
            (join_in, j_send_sem, j_recv_sem.at[0], twin(1))]
    if teams > 1:
        drains += [
            (deal_in, d_send_sem, d_recv_sem, ally(1)), (cross_in_step, cs_send_sem, cs_recv_sem.at[0], ally(1)),
            (cross_in, c_send_sem, c_recv_sem.at[0], ally(1))]
    if twinned:
        drains += [
            (twin_in_step, ts_send_sem, ts_recv_sem.at[0], twin(1)), (twin_in, t_send_sem, t_recv_sem.at[0], twin(1))]
    for ref, send_sem, recv_sem, device in drains:
        remote(ref, ref, send_sem, recv_sem, device).wait_send()
    arrivals = []
    if len(twinned) < chunks:
        arrivals += [(ret_scale, s_send_sem, s_recv_sem), (ret, r_send_sem, r_recv_sem)]
    if twinned:
        arrivals += [(pair_scale, bs_send_sem, bs_recv_sem), (pair, b_send_sem, b_recv_sem)]
    for ref, send_sem, recv_sem in arrivals:
        remote(ref, ref, send_sem, recv_sem, fellow_any).wait_recv()
    for q in range(plane):
        scales = jnp.concatenate([scale_ref[q, l] for l in range(levels)], axis=0)
        for k in range(chunks):
            spread_ref[q, :, lanes(k)] = spread(scales[:, k * LANES:(k + 1) * LANES], wide)
    for ref, send_sem, recv_sem in arrivals:
        remote(ref, ref, send_sem, recv_sem, fellow_any).wait_send()


def local(gradients, token_counts, row_groups, col_groups):
    rows, cols = lax.axis_size("row"), lax.axis_size("col")
    across = 2 if rows % 2 == 0 else 1
    depth, plane = rows // across, across * cols
    width = gradients.shape[-1]
    lines = gradients.size // width
    levels = 2 if depth % 2 == 0 and lines % (2 * plane * 16) == 0 else 1
    teams = depth // levels
    height = lines // (plane * levels)
    wide = WIDE if width % WIDE == 0 else LANES
    chunks = width // wide
    groups = cols
    counts = jnp.broadcast_to(token_counts.astype(F32), (1, LANES))
    pieces = gradients.reshape(plane, levels, height, width)
    hbm = pl.BlockSpec(memory_space=pltpu.HBM)
    stay = functools.partial(pltpu.with_memory_space_constraint, memory_space=pltpu.HBM)
    vmem = pl.BlockSpec(memory_space=pltpu.VMEM)
    others, mates = max(teams - 1, 1), max(levels - 1, 1)
    joined = tuple(k for k in JOINED if k < chunks and levels > 1)
    twinned = tuple(k for k in TWINNED if k < chunks and levels > 1)
    rest, raw = max(len(joined), 1), max(chunks - len(joined), 1)
    paired, single = max(len(twinned), 1), max(chunks - len(twinned), 1)
    crew = levels * plane
    sem = pltpu.SemaphoreType.DMA
    codes, scales, total = pl.pallas_call(
        functools.partial(kernel, (across, cols, depth, levels, chunks, joined, twinned, wide)),
        out_shape=(
            jax.ShapeDtypeStruct((plane, levels, height, width), jnp.int16),
            jax.ShapeDtypeStruct((plane, levels, width), F32),
            jax.ShapeDtypeStruct((1, LANES), F32),
        ),
        in_specs=[hbm, hbm, vmem, hbm],
        out_specs=(vmem, vmem, vmem),
        scratch_shapes=[
            pltpu.VMEM((plane, levels, 1, chunks * LANES), F32),
            pltpu.SMEM((2, cols, rows), jnp.int32),
            pltpu.SMEM((1, cols, rows), jnp.int32),
            pltpu.VMEM((plane, levels, height, width), gradients.dtype),
            pltpu.VMEM((rest, plane - 1, levels, height, wide), gradients.dtype),
            pltpu.VMEM((raw, crew - 1, height, wide), gradients.dtype),
            pltpu.VMEM((chunks, groups, height, wide), F32),
            pltpu.VMEM((rest, mates, groups, height, wide), jnp.int16),
            pltpu.VMEM((rest, mates, groups, 1, LANES), F32),
            pltpu.VMEM((rest, mates, groups, height, wide), jnp.int16),
            pltpu.VMEM((rest, mates, groups, 1, LANES), F32),
            pltpu.VMEM((chunks, groups, height, wide), jnp.int16),
            pltpu.VMEM((chunks, groups, 1, LANES), F32),
            pltpu.VMEM((chunks, others, groups, height, wide), jnp.int16),
            pltpu.VMEM((chunks, others, groups, 1, LANES), F32),
            pltpu.VMEM((groups, height, wide), jnp.int16),
            pltpu.VMEM((groups, 1, LANES), F32),
            pltpu.VMEM((single, crew - 1, height, wide), jnp.int16),
            pltpu.VMEM((single, crew - 1, 1, LANES), F32),
            pltpu.VMEM((paired, groups, height, wide), jnp.int16),
            pltpu.VMEM((paired, groups, 1, LANES), F32),
            pltpu.VMEM((paired, mates, groups, height, wide), jnp.int16),
            pltpu.VMEM((paired, mates, groups, 1, LANES), F32),
            pltpu.VMEM((levels, groups, height, wide), jnp.int16),
            pltpu.VMEM((levels, groups, 1, LANES), F32),
            pltpu.VMEM((paired, plane - 1, levels, height, wide), jnp.int16),
            pltpu.VMEM((paired, plane - 1, levels, 1, LANES), F32),
            pltpu.VMEM((1, LANES), F32),
            pltpu.VMEM((crew - 1, 1, LANES), F32),
            pltpu.VMEM((groups, 1, LANES), F32),
            pltpu.VMEM((others, groups, 1, LANES), F32),
            pltpu.VMEM((groups, 1, LANES), F32),
            pltpu.VMEM((groups, 1, LANES), F32),
            pltpu.VMEM((crew, groups, 1, wide), F32),
            pltpu.SMEM((rows, groups), jnp.int32),
            pltpu.SMEM((rows, groups), jnp.int32),
            pltpu.SMEM((groups, groups), jnp.int32),
            pltpu.SMEM((crew,), jnp.int32),
            sem((3,)), sem, sem((chunks,)), sem, sem, sem, sem,
            sem, sem((rest,)), sem, sem((rest,)),
            sem, sem((chunks,)), sem, sem((chunks,)), sem, sem((paired,)), sem, sem((paired,)),
            sem, sem, sem, sem, sem, sem, sem, sem,
        ],
        compiler_params=pltpu.CompilerParams(
            collective_id=0, has_side_effects=True, vmem_limit_bytes=VMEM_GRANT
        ),
    )(stay(jnp.swapaxes(row_groups, 1, 2)), stay(col_groups), counts, stay(pieces))
    averaged = codes.astype(F32) * scales[:, :, None, :]
    return averaged.reshape(gradients.shape), jnp.max(total.astype(jnp.int32), axis=1, keepdims=True)


def solution(mesh):
    placed = (P("row", "col", None, None, None), P("row", "col"), P(), P())
    return jax.shard_map(
        local,
        mesh=mesh,
        in_specs=placed,
        out_specs=(P("row", "col", None, None, None), P("row", "col")),
        check_vma=False,
    )
```

```python
import functools

import jax
import jax.numpy as jnp
from jax import lax
from jax.experimental import pallas as pl
from jax.experimental.pallas import tpu as pltpu
from jax.sharding import PartitionSpec as P

MESH = pl.DeviceIdType.MESH
F32 = jnp.float32
WIDE = 256
JOINED = ()
TWINNED = (0, 1)
LEAD = 6.5
FAR = 4.6
JOIN_LAG = 2.2
CROSS_LAG = 2.6
TWIN_LAG = 2.2
VMEM_GRANT = 48 * 1024 * 1024
LIMIT = 32766.0
SMALLEST = 1e-33
LANES = 128


def add(one, two):
    return one + two


def path_counts(cols, table, between, second, third, paths):
    hops = between.shape[2]

    @pl.loop(0, hops)
    def _(h):
        for g in range(cols):
            for turn, into in ((0, second), (1, third)):
                into[h, g] = functools.reduce(add, [
                    (table[turn, g, between[0, j, h]] == j).astype(jnp.int32) for j in range(cols)])

    @pl.loop(0, cols)
    def _(k):
        for g in range(cols):
            paths[k, g] = functools.reduce(add, [third[h, k] * second[h, g] for h in range(hops)])


def group_of(table, turn, row, col, cols):
    found = jnp.int32(0)
    for g in range(cols):
        found = jnp.where(table[turn, g, row] == col, g, found)
    return found


def spread(row, wide):
    return jnp.concatenate([row] * (wide // LANES), axis=1)


def quantize(part):
    wide = part.shape[1]
    top = jnp.max(jnp.abs(part), axis=0, keepdims=True)
    top = functools.reduce(jnp.maximum, [top[:, low:low + LANES] for low in range(0, wide, LANES)])
    step = jnp.maximum(top, SMALLEST) * (1.0 / LIMIT)
    return jnp.round(part * spread(1.0 / step, wide)).astype(jnp.int32).astype(jnp.int16), step


def encode(sums, code_ref, step_ref):
    for g, part in enumerate(sums):
        code_ref[g], step_ref[g] = quantize(part)


def decode(groups, code_ref, step_ref):
    wide = code_ref.shape[-1]
    return [code_ref[g].astype(F32) * spread(step_ref[g], wide) for g in range(groups)]


def kernel(
    geometry,
    table_hbm, between_hbm, count_ref, x_hbm,
    out_ref, spread_ref, total_ref,
    scale_ref, table, between, x_ref,
    recv, recv_raw, own, join_out, join_out_step, join_in, join_in_step, cross_out, cross_out_step, cross_in, cross_in_step,
    codes, steps, ret, ret_scale, twin_out, twin_out_step, twin_in, twin_in_step, pick, pick_step, pair, pair_scale,
    cnt_out, cnt_in, deal_out, deal_in, weights, inverse, factor,
    second, third, paths, chosen,
    load_sem, x_send_sem, x_recv_sem, n_send_sem, n_recv_sem, d_send_sem, d_recv_sem,
    j_send_sem, j_recv_sem, js_send_sem, js_recv_sem,
    c_send_sem, c_recv_sem, cs_send_sem, cs_recv_sem, t_send_sem, t_recv_sem, ts_send_sem, ts_recv_sem,
    r_send_sem, r_recv_sem, s_send_sem, s_recv_sem, b_send_sem, b_recv_sem, bs_send_sem, bs_recv_sem,
):
    across, cols, depth, levels, chunks, joined, twinned, wide = geometry
    crew = levels * across * cols
    slot = {k: (joined.index(k) if k in joined else k - sum(j < k for j in joined)) for k in range(chunks)}
    berth = {k: (twinned.index(k) if k in twinned else k - sum(j < k for j in twinned)) for k in range(chunks)}
    plane, teams, groups = across * cols, depth // levels, cols
    row, col = lax.axis_index("row"), lax.axis_index("col")
    z = row // across
    team, deck = z // levels, z % levels
    spot = (row % across) * cols + col

    def at(level, q):
        return (level * across + q // cols, q % cols)

    def fellow(q):
        return at(z, q)

    def mate(n):
        return at(team * levels + (deck + n // plane) % levels, (spot + n) % plane)

    def ally(d):
        return at((team + d) % teams * levels + deck, spot)

    def twin(d):
        return at(team * levels + (deck + d) % levels, spot)

    def lanes(k):
        return pl.ds(k * wide, wide)

    def remote(src, dst, send_sem, recv_sem, device):
        return pltpu.make_async_remote_copy(
            src_ref=src, dst_ref=dst, send_sem=send_sem, recv_sem=recv_sem, device_id=device, device_id_type=MESH)

    loads = [
        pltpu.make_async_copy(src, dst, load_sem.at[n])
        for n, (src, dst) in enumerate(
            [(x_hbm, x_ref), (table_hbm, table), (between_hbm, between)])]
    for load in loads:
        load.start()

    barrier = pltpu.get_barrier_semaphore()
    for n in range(1, crew):
        pl.semaphore_signal(barrier, inc=1, device_id=mate(n), device_id_type=MESH)
    for d in range(1, teams):
        pl.semaphore_signal(barrier, inc=1, device_id=ally(d), device_id_type=MESH)
    cnt_out[...] = count_ref[...]
    loads[0].wait()
    pl.semaphore_wait(barrier, crew + teams - 2)

    def strips(k):
        return pl.ds(k * LANES, LANES)

    def count_copy(n):
        return remote(cnt_out, cnt_in.at[n - 1], n_send_sem, n_recv_sem, mate(n))

    def piece_copy(k, d):
        to = (spot + d) % plane
        return remote(x_ref.at[to, :, :, lanes(k)], recv.at[slot[k], d - 1], x_send_sem, x_recv_sem.at[k], fellow(to))

    def raw_copy(k, n):
        source = x_ref.at[(spot + n) % plane, (deck + n // plane) % levels, :, lanes(k)]
        return remote(source, recv_raw.at[slot[k], n - 1], x_send_sem, x_recv_sem.at[k], mate(n))

    def deal_copy(d):
        return remote(deal_out, deal_in.at[d - 1], d_send_sem, d_recv_sem, ally(d))

    def join_copies(k, d):
        return (
            remote(join_out_step.at[slot[k], d - 1], join_in_step.at[slot[k], d - 1], js_send_sem, js_recv_sem.at[slot[k]], twin(d)),
            remote(join_out.at[slot[k], d - 1], join_in.at[slot[k], d - 1], j_send_sem, j_recv_sem.at[slot[k]], twin(d)))

    def cross_copies(k, d):
        return (
            remote(cross_out_step.at[k], cross_in_step.at[k, d - 1], cs_send_sem, cs_recv_sem.at[k], ally(d)),
            remote(cross_out.at[k], cross_in.at[k, d - 1], c_send_sem, c_recv_sem.at[k], ally(d)))

    def return_copies(k, n):
        i = berth[k]
        return (
            remote(ret_scale.at[i, n - 1], scale_ref.at[spot, deck, :, strips(k)], s_send_sem, s_recv_sem, mate(n)),
            remote(ret.at[i, n - 1], out_ref.at[spot, deck, :, lanes(k)], r_send_sem, r_recv_sem, mate(n)))

    def twin_copies(k, d):
        i = berth[k]
        return (
            remote(twin_out_step.at[i], twin_in_step.at[i, d - 1], ts_send_sem, ts_recv_sem.at[i], twin(d)),
            remote(twin_out.at[i], twin_in.at[i, d - 1], t_send_sem, t_recv_sem.at[i], twin(d)))

    def pair_copies(k, d):
        i, to = berth[k], fellow((spot + d) % plane)
        return (
            remote(pair_scale.at[i, d - 1], scale_ref.at[spot, :, :, strips(k)], bs_send_sem, bs_recv_sem, to),
            remote(pair.at[i, d - 1], out_ref.at[spot, :, :, lanes(k)], b_send_sem, b_recv_sem, to))

    def begin(k):
        if k not in joined:
            for n in range(1, plane):
                raw_copy(k, n).start()
        else:
            for d in range(1, plane):
                piece_copy(k, d).start()

    def begin_far(k):
        for n in range(plane, crew if k not in joined else 0):
            raw_copy(k, n).start()

    def gather_raw(k):
        remote(recv_raw.at[slot[k]], recv_raw.at[slot[k]], x_send_sem, x_recv_sem.at[k], fellow_any).wait_recv()
        sums = weigh([x_ref[spot, deck, :, lanes(k)] if n == 0 else recv_raw[slot[k], n - 1] for n in range(crew)])
        for g in range(groups):
            own[k, g] = sums[g]
        send_cross(k, sums)

    def weigh(pieces):
        sums = [None] * groups
        for n, piece in enumerate(pieces):
            piece = piece.astype(F32)
            for g in range(groups):
                term = piece * factor[n, g]
                sums[g] = term if n == 0 else sums[g] + term
        return sums

    def send_cross(k, sums):
        if teams > 1:
            encode(sums, cross_out.at[k], cross_out_step.at[k])
            for d in range(1, teams):
                for copy in cross_copies(k, d):
                    copy.start()

    def gather(k):
        remote(recv.at[slot[k]], recv.at[slot[k]], x_send_sem, x_recv_sem.at[k], fellow_any).wait_recv()
        for o in reversed(range(levels)):
            rows = (deck + o) % levels
            sums = weigh(
                [x_ref[spot, rows, :, lanes(k)] if d == 0 else recv[slot[k], d - 1, rows] for d in range(plane)])
            if o > 0:
                encode(sums, join_out.at[slot[k], o - 1], join_out_step.at[slot[k], o - 1])
                for copy in join_copies(k, o):
                    copy.start()
            else:
                for g in range(groups):
                    own[k, g] = sums[g]

    def join(k):
        sums = [own[k, g] for g in range(groups)]
        if levels > 1:
            remote(join_in_step.at[slot[k]], join_in_step.at[slot[k]], js_send_sem, js_recv_sem.at[slot[k]], twin(1)).wait_recv()
            remote(join_in.at[slot[k]], join_in.at[slot[k]], j_send_sem, j_recv_sem.at[slot[k]], twin(1)).wait_recv()
            for d in range(1, levels):
                sums = [a + b for a, b in zip(sums, decode(groups, join_in.at[slot[k], d - 1], join_in_step.at[slot[k], d - 1]))]
            for g in range(groups):
                own[k, g] = sums[g]
        send_cross(k, sums)

    def settle():
        for n in range(crew):
            chosen[n] = group_of(table, 1, *mate(n), cols)
        if teams > 1:
            remote(deal_in, deal_in, d_send_sem, d_recv_sem, ally(1)).wait_recv()
        for g in range(groups):
            weight = deal_out[g]
            for d in range(1, teams):
                weight = weight + deal_in[d - 1, g]
            weights[g] = weight
            inverse[g] = 1.0 / weight
        total_ref[...] = weights[chosen[0]]

    def cross(k):
        sums = [own[k, g] for g in range(groups)]
        if teams > 1:
            remote(cross_in_step.at[k], cross_in_step.at[k], cs_send_sem, cs_recv_sem.at[k], ally(1)).wait_recv()
            remote(cross_in.at[k], cross_in.at[k], c_send_sem, c_recv_sem.at[k], ally(1)).wait_recv()
        for d in range(1, teams):
            sums = [a + b for a, b in zip(sums, decode(groups, cross_in.at[k, d - 1], cross_in_step.at[k, d - 1]))]
        i = berth[k]
        for g in range(groups):
            code, step = quantize(sums[g] * spread(inverse[g], wide))
            if k in twinned:
                twin_out[i, g], twin_out_step[i, g] = code, step
            else:
                codes[g], steps[g] = code, step
        if k in twinned:
            for d in range(1, levels):
                for copy in twin_copies(k, d):
                    copy.start()
            return
        for n in range(1, crew):
            ret[i, n - 1] = codes[chosen[n]]
            ret_scale[i, n - 1] = steps[chosen[n]]
            for copy in return_copies(k, n):
                copy.start()
        out_ref[spot, deck, :, lanes(k)] = codes[chosen[0]]
        scale_ref[spot, deck, :, strips(k)] = steps[chosen[0]]

    def give(k):
        i = berth[k]
        remote(twin_in_step.at[i], twin_in_step.at[i], ts_send_sem, ts_recv_sem.at[i], twin(1)).wait_recv()
        remote(twin_in.at[i], twin_in.at[i], t_send_sem, t_recv_sem.at[i], twin(1)).wait_recv()
        for g in range(groups):
            pick[0, g], pick_step[0, g] = twin_out[i, g], twin_out_step[i, g]
            for d in range(1, levels):
                pick[d, g], pick_step[d, g] = twin_in[i, d - 1, g], twin_in_step[i, d - 1, g]
        for d in range(plane):
            for l in range(levels):
                home = (deck + levels - l) % levels
                code, step = pick[l, chosen[d]], pick_step[l, chosen[d]]
                if d == 0:
                    out_ref[spot, home, :, lanes(k)] = code
                    scale_ref[spot, home, :, strips(k)] = step
                else:
                    pair[i, d - 1, home] = code
                    pair_scale[i, d - 1, home] = step
            if d > 0:
                for copy in pair_copies(k, d):
                    copy.start()

    fellow_any = fellow((spot + 1) % plane)
    for n in range(1, crew):
        count_copy(n).start()
    plan = []
    for k in range(chunks):
        plan.append((k - LEAD, 0, begin, k))
        plan.append((k - FAR, 0, begin_far, k))
        lag = k
        if k in joined:
            plan.append((lag, 4, gather, k))
            lag += JOIN_LAG
            plan.append((lag, 3, join, k))
        else:
            plan.append((lag, 4, gather_raw, k))
        lag += CROSS_LAG
        plan.append((lag, 2, cross, k))
        if k in twinned:
            plan.append((lag + TWIN_LAG, 1, give, k))
    plan.sort(key=lambda entry: (entry[0], entry[1]))
    early = [entry for entry in plan if entry[0] < 0]
    for _, _, action, k in early:
        action(k)

    loads[1].wait()
    loads[2].wait()
    path_counts(cols, table, between, second, third, paths)
    remote(cnt_in, cnt_in, n_send_sem, n_recv_sem, fellow_any).wait_recv()
    parts = [None] * groups
    for n in range(crew):
        i, j = at(team * levels + (deck + levels - n // plane) % levels, (spot + plane - n % plane) % plane)
        first = group_of(table, 0, i, j, cols)
        tally = cnt_out[...] if n == 0 else cnt_in[n - 1]
        for g in range(groups):
            term = paths[g, first].astype(F32) * tally
            factor[n, g] = spread(term, wide)
            parts[g] = term if n == 0 else parts[g] + term
    for g in range(groups):
        deal_out[g] = parts[g]
    for d in range(1, teams):
        deal_copy(d).start()

    seen = set()
    for _, _, action, k in plan[len(early):]:
        if action is cross and cross not in seen:
            settle()
        seen.add(action)
        action(k)

    remote(cnt_in, cnt_in, n_send_sem, n_recv_sem, fellow_any).wait_send()
    drains = []
    if len(joined) < chunks:
        drains.append((recv_raw, x_send_sem, x_recv_sem.at[0], fellow_any))
    if joined:
        drains += [
            (recv, x_send_sem, x_recv_sem.at[0], fellow_any), (join_in_step, js_send_sem, js_recv_sem.at[0], twin(1)),
            (join_in, j_send_sem, j_recv_sem.at[0], twin(1))]
    if teams > 1:
        drains += [
            (deal_in, d_send_sem, d_recv_sem, ally(1)), (cross_in_step, cs_send_sem, cs_recv_sem.at[0], ally(1)),
            (cross_in, c_send_sem, c_recv_sem.at[0], ally(1))]
    if twinned:
        drains += [
            (twin_in_step, ts_send_sem, ts_recv_sem.at[0], twin(1)), (twin_in, t_send_sem, t_recv_sem.at[0], twin(1))]
    for ref, send_sem, recv_sem, device in drains:
        remote(ref, ref, send_sem, recv_sem, device).wait_send()
    arrivals = []
    if len(twinned) < chunks:
        arrivals += [(ret_scale, s_send_sem, s_recv_sem), (ret, r_send_sem, r_recv_sem)]
    if twinned:
        arrivals += [(pair_scale, bs_send_sem, bs_recv_sem), (pair, b_send_sem, b_recv_sem)]
    for ref, send_sem, recv_sem in arrivals:
        remote(ref, ref, send_sem, recv_sem, fellow_any).wait_recv()
    for q in range(plane):
        scales = jnp.concatenate([scale_ref[q, l] for l in range(levels)], axis=0)
        for k in range(chunks):
            spread_ref[q, :, lanes(k)] = spread(scales[:, k * LANES:(k + 1) * LANES], wide)
    for ref, send_sem, recv_sem in arrivals:
        remote(ref, ref, send_sem, recv_sem, fellow_any).wait_send()


def local(gradients, token_counts, row_groups, col_groups):
    rows, cols = lax.axis_size("row"), lax.axis_size("col")
    across = 2 if rows % 2 == 0 else 1
    depth, plane = rows // across, across * cols
    width = gradients.shape[-1]
    lines = gradients.size // width
    levels = 2 if depth % 2 == 0 and lines % (2 * plane * 16) == 0 else 1
    teams = depth // levels
    height = lines // (plane * levels)
    wide = WIDE if width % WIDE == 0 else LANES
    chunks = width // wide
    groups = cols
    counts = jnp.broadcast_to(token_counts.astype(F32), (1, LANES))
    pieces = gradients.reshape(plane, levels, height, width)
    hbm = pl.BlockSpec(memory_space=pltpu.HBM)
    stay = functools.partial(pltpu.with_memory_space_constraint, memory_space=pltpu.HBM)
    vmem = pl.BlockSpec(memory_space=pltpu.VMEM)
    others, mates = max(teams - 1, 1), max(levels - 1, 1)
    joined = tuple(k for k in JOINED if k < chunks and levels > 1)
    twinned = tuple(k for k in TWINNED if k < chunks and levels > 1)
    rest, raw = max(len(joined), 1), max(chunks - len(joined), 1)
    paired, single = max(len(twinned), 1), max(chunks - len(twinned), 1)
    crew = levels * plane
    sem = pltpu.SemaphoreType.DMA
    codes, scales, total = pl.pallas_call(
        functools.partial(kernel, (across, cols, depth, levels, chunks, joined, twinned, wide)),
        out_shape=(
            jax.ShapeDtypeStruct((plane, levels, height, width), jnp.int16),
            jax.ShapeDtypeStruct((plane, levels, width), F32),
            jax.ShapeDtypeStruct((1, LANES), F32),
        ),
        in_specs=[hbm, hbm, vmem, hbm],
        out_specs=(vmem, vmem, vmem),
        scratch_shapes=[
            pltpu.VMEM((plane, levels, 1, chunks * LANES), F32),
            pltpu.SMEM((2, cols, rows), jnp.int32),
            pltpu.SMEM((1, cols, rows), jnp.int32),
            pltpu.VMEM((plane, levels, height, width), gradients.dtype),
            pltpu.VMEM((rest, plane - 1, levels, height, wide), gradients.dtype),
            pltpu.VMEM((raw, crew - 1, height, wide), gradients.dtype),
            pltpu.VMEM((chunks, groups, height, wide), F32),
            pltpu.VMEM((rest, mates, groups, height, wide), jnp.int16),
            pltpu.VMEM((rest, mates, groups, 1, LANES), F32),
            pltpu.VMEM((rest, mates, groups, height, wide), jnp.int16),
            pltpu.VMEM((rest, mates, groups, 1, LANES), F32),
            pltpu.VMEM((chunks, groups, height, wide), jnp.int16),
            pltpu.VMEM((chunks, groups, 1, LANES), F32),
            pltpu.VMEM((chunks, others, groups, height, wide), jnp.int16),
            pltpu.VMEM((chunks, others, groups, 1, LANES), F32),
            pltpu.VMEM((groups, height, wide), jnp.int16),
            pltpu.VMEM((groups, 1, LANES), F32),
            pltpu.VMEM((single, crew - 1, height, wide), jnp.int16),
            pltpu.VMEM((single, crew - 1, 1, LANES), F32),
            pltpu.VMEM((paired, groups, height, wide), jnp.int16),
            pltpu.VMEM((paired, groups, 1, LANES), F32),
            pltpu.VMEM((paired, mates, groups, height, wide), jnp.int16),
            pltpu.VMEM((paired, mates, groups, 1, LANES), F32),
            pltpu.VMEM((levels, groups, height, wide), jnp.int16),
            pltpu.VMEM((levels, groups, 1, LANES), F32),
            pltpu.VMEM((paired, plane - 1, levels, height, wide), jnp.int16),
            pltpu.VMEM((paired, plane - 1, levels, 1, LANES), F32),
            pltpu.VMEM((1, LANES), F32),
            pltpu.VMEM((crew - 1, 1, LANES), F32),
            pltpu.VMEM((groups, 1, LANES), F32),
            pltpu.VMEM((others, groups, 1, LANES), F32),
            pltpu.VMEM((groups, 1, LANES), F32),
            pltpu.VMEM((groups, 1, LANES), F32),
            pltpu.VMEM((crew, groups, 1, wide), F32),
            pltpu.SMEM((rows, groups), jnp.int32),
            pltpu.SMEM((rows, groups), jnp.int32),
            pltpu.SMEM((groups, groups), jnp.int32),
            pltpu.SMEM((crew,), jnp.int32),
            sem((3,)), sem, sem((chunks,)), sem, sem, sem, sem,
            sem, sem((rest,)), sem, sem((rest,)),
            sem, sem((chunks,)), sem, sem((chunks,)), sem, sem((paired,)), sem, sem((paired,)),
            sem, sem, sem, sem, sem, sem, sem, sem,
        ],
        compiler_params=pltpu.CompilerParams(
            collective_id=0, has_side_effects=True, vmem_limit_bytes=VMEM_GRANT
        ),
    )(stay(jnp.swapaxes(row_groups, 1, 2)), stay(col_groups), counts, stay(pieces))
    averaged = codes.astype(F32) * scales[:, :, None, :]
    return averaged.reshape(gradients.shape), jnp.max(total.astype(jnp.int32), axis=1, keepdims=True)


def solution(mesh):
    placed = (P("row", "col", None, None, None), P("row", "col"), P(), P())
    return jax.shard_map(
        local,
        mesh=mesh,
        in_specs=placed,
        out_specs=(P("row", "col", None, None, None), P("row", "col")),
        check_vma=False,
    )
```
